32 devices in a mesh: ctx: 8 (over y, x, core), head: 4 (over z).
Axes of the slice: x: 2, y: 2, z: 4, core: 2. Of those that a mesh axis runs over, the one named last changes fastest.
Arguments:
- query_nope: bfloat16 [1024, 8192], P('ctx', 'head'), may hold values from -6 to 6
- query_rope: bfloat16 [1024, 4096], P('ctx', 'head'), may hold values from -450 to 450
- grad_out: bfloat16 [1024, 8192], P('ctx', 'head'), may hold values from -24 to 24
- latent: bfloat16 [1024, 576], P(('ctx', 'head')), may hold values from -8 to 8
- key_up: bfloat16 [512, 8192], P(None, 'head'), may hold values from -0.25 to 0.25
- value_up: bfloat16 [512, 8192], P(None, 'head'), may hold values from -0.25 to 0.25
- block_keep: int32 [8, 3], P('ctx'), may hold values 0 or 1
Outputs:
- d_query_nope: float32 [1024, 8192], P('ctx', 'head')
- d_query_rope: float32 [1024, 4096], P('ctx', 'head')
- d_latent: float32 [1024, 576], P(('ctx', 'head'))
The draws below stay inside these ranges and needn't reach their ends.
All inputs are finite; a program needn't handle non-finite values. No bound on the sum of `block_keep` on one device may be relied on, other than what follows from the above.
Results may differ from the reference program's by a relative error of at most 0.015.
Values may be sent and summed in bfloat16 or wider, within the bound.
A program may use at most 64 MiB of HBM per device.

```python
import math
import jax
import jax.numpy as jnp
from jax import lax

HEADS = 64
NOPE = 128
ROPE = 64
VDIM = 128
RANK = 512
STEPS = 3
GROUP = 128
LATENT = 576
TOKENS = 1024
NBLOCKS = 8
N_CTX = 8


def draw_latent(key, part):
    drawn = jnp.clip(jax.random.normal(jax.random.fold_in(key, 1), (TOKENS, LATENT), jnp.float32), -6.0, 6.0)
    return drawn.astype(jnp.bfloat16)


def draw_query_rope(key, part):
    drawn = jnp.clip(jax.random.normal(jax.random.fold_in(key, 3), (TOKENS, HEADS * ROPE), jnp.float32), -6.0, 6.0)
    return drawn.astype(jnp.bfloat16)


def draw_query_nope(key, part):
    drawn = jnp.clip(jax.random.normal(jax.random.fold_in(key, 5), (TOKENS, HEADS * NOPE), jnp.float32), -6.0, 6.0)
    return drawn.astype(jnp.bfloat16)


def set_ends(values, own_key, low, high):
    longest = values.shape.index(max(values.shape))
    spots = []
    for shift in (0, 1):
        where = [jax.random.randint(jax.random.fold_in(own_key, axis), (), 0, length) for axis, length in enumerate(values.shape)]
        where[longest] = (where[longest] + shift) % values.shape[longest]
        spots.append(tuple(where))
    return values.at[spots[0]].set(low).at[spots[1]].set(high)


def levels(own_key, dims, split, low, high):
    loudness, own = 1.0, jax.random.fold_in(own_key, 6)
    for dim, shards_of in split:
        heights = jnp.exp(jax.random.uniform(jax.random.fold_in(own, dim), (shards_of,), jnp.float32, low / len(split), high / len(split)))
        loudness = loudness * jnp.repeat(heights, dims[dim] // shards_of).reshape([-1 if axis == dim else 1 for axis in range(len(dims))])
    return loudness


def scatter_about(stream_key, dims, width, limit, split=(), held_as=jnp.bfloat16):
    factor_of = levels(stream_key, dims, split, -0.22, 0.18) if split else 1.0
    array = jax.random.normal(stream_key, dims, jnp.float32) * width * factor_of
    return jnp.minimum(jnp.maximum(array, -limit), limit).astype(held_as)


def setup_inputs(seed: int = 0) -> dict:
    seeds = jax.random.split(jax.random.key(seed), 8)
    query_nope = draw_query_nope(jax.random.fold_in(seeds[7], 71), 0)
    query_rope = draw_query_rope(jax.random.fold_in(seeds[7], 71), 0)
    grad_out = scatter_about(seeds[2], (TOKENS, HEADS * VDIM), 4.0, 24.0, ((0, 8), (1, 4)))
    latent = draw_latent(jax.random.fold_in(seeds[7], 71), 0)
    key_up = scatter_about(seeds[4], (RANK, HEADS * NOPE), RANK ** -0.5, 0.25, ((1, 4),))
    value_up = scatter_about(seeds[5], (RANK, HEADS * VDIM), RANK ** -0.5, 0.25, ((1, 4),))
    block_keep = set_ends((jax.random.randint(seeds[6], (NBLOCKS, STEPS), 0, 4) < 3).astype(jnp.int32), jax.random.fold_in(seeds[6], 1), 0, 1)
    return {"query_nope": query_nope, "query_rope": query_rope, "grad_out": grad_out, "latent": latent, "key_up": key_up, "value_up": value_up, "block_keep": block_keep}


def window_mask(group_len, cycle_steps, keep_row, position):
    grid_shape = (group_len, cycle_steps + 1, group_len)
    query_at = lax.broadcasted_iota(jnp.int32, grid_shape, 0)
    block_at = lax.broadcasted_iota(jnp.int32, grid_shape, 1)
    key_at = lax.broadcasted_iota(jnp.int32, grid_shape, 2)
    blocks_back = cycle_steps - block_at
    block_flags = jnp.concatenate([keep_row[::-1], jnp.ones((1,), jnp.int32)])
    kept_block = block_flags[None, :, None] == 1
    in_range = position - blocks_back >= 0
    causal = (blocks_back > 0) | (key_at <= query_at)
    return (kept_block & in_range & causal).reshape(group_len, (cycle_steps + 1) * group_len)

def block_grads(query_nope, query_rope, grad_out, keys_nope, values, keys_rope, key_up, value_up, allowed):
    group_len = query_nope.shape[0]
    window_len = keys_nope.shape[0]
    head_count = key_up.shape[1] // NOPE
    score_scale = 1.0 / math.sqrt(NOPE + ROPE)
    query_heads = query_nope.reshape(group_len, head_count, NOPE).astype(jnp.float32)
    rope_heads = query_rope.reshape(group_len, head_count, ROPE).astype(jnp.float32)
    out_heads = grad_out.reshape(group_len, head_count, VDIM).astype(jnp.float32)
    key_heads = keys_nope.reshape(window_len, head_count, NOPE).astype(jnp.float32)
    value_heads = values.reshape(window_len, head_count, VDIM).astype(jnp.float32)
    rope_keys = keys_rope.astype(jnp.float32)
    scores = (jnp.einsum('chd,khd->hck', query_heads, key_heads) + jnp.einsum('chd,kd->hck', rope_heads, rope_keys)) * score_scale
    scores = jnp.where(allowed[None], scores, -jnp.inf)
    row_top = lax.optimization_barrier(jnp.max(scores, axis=2, keepdims=True))
    exponent = jnp.exp(scores - row_top)
    probs = exponent / lax.optimization_barrier(jnp.sum(exponent, axis=2, keepdims=True))
    weights = probs.astype(jnp.bfloat16)
    output = jnp.einsum('hck,khd->chd', weights.astype(jnp.float32), value_heads)
    row_delta = lax.optimization_barrier(jnp.sum(output * out_heads, axis=2))
    slopes = jnp.einsum('chd,khd->hck', out_heads, value_heads)
    score_grad = (probs * (slopes - row_delta.T[:, :, None]) * score_scale).astype(jnp.bfloat16)
    grad_f32 = score_grad.astype(jnp.float32)
    query_grad_nope = jnp.einsum('hck,khd->chd', grad_f32, key_heads).reshape(group_len, head_count * NOPE)
    query_grad_rope = jnp.einsum('hck,kd->chd', grad_f32, rope_keys).reshape(group_len, head_count * ROPE)
    key_grad = jnp.einsum('hck,chd->khd', grad_f32, query_heads).astype(jnp.bfloat16).reshape(window_len, head_count * NOPE)
    rope_grad = jnp.einsum('hck,chd->kd', grad_f32, rope_heads)
    value_grad = jnp.einsum('hck,chd->khd', weights.astype(jnp.float32), out_heads).astype(jnp.bfloat16).reshape(window_len, head_count * VDIM)
    content_grad = jnp.dot(key_grad, key_up.T, preferred_element_type=jnp.float32) + jnp.dot(value_grad, value_up.T, preferred_element_type=jnp.float32)
    return (query_grad_nope, query_grad_rope, jnp.concatenate([content_grad, rope_grad], axis=1))

def reference(query_nope, query_rope, grad_out, latent, key_up, value_up, block_keep):
    content = latent[:, :RANK]
    keys_nope = jnp.dot(content, key_up, preferred_element_type=jnp.float32).astype(jnp.bfloat16)
    values = jnp.dot(content, value_up, preferred_element_type=jnp.float32).astype(jnp.bfloat16)
    keys_rope = latent[:, RANK:]
    lead_rows = STEPS * GROUP
    window_len = (STEPS + 1) * GROUP

    def pad_front(source_rows):
        return jnp.concatenate([jnp.zeros((lead_rows, source_rows.shape[1]), source_rows.dtype), source_rows], axis=0)
    padded_nope = pad_front(keys_nope)
    padded_values = pad_front(values)
    padded_rope = pad_front(keys_rope)

    def one_block(carried, block_index):
        row_start = (block_index * GROUP).astype(jnp.int32)
        query_rows = lax.dynamic_slice_in_dim(query_nope, row_start, GROUP, 0)
        rope_rows = lax.dynamic_slice_in_dim(query_rope, row_start, GROUP, 0)
        out_rows = lax.dynamic_slice_in_dim(grad_out, row_start, GROUP, 0)
        window_nope = lax.dynamic_slice_in_dim(padded_nope, row_start, window_len, 0)
        window_values = lax.dynamic_slice_in_dim(padded_values, row_start, window_len, 0)
        window_rope = lax.dynamic_slice_in_dim(padded_rope, row_start, window_len, 0)
        keep_row = lax.dynamic_index_in_dim(block_keep, block_index, 0, keepdims=False)
        allowed = window_mask(GROUP, STEPS, keep_row, block_index)
        grad_nope, grad_rope, partial_value = block_grads(query_rows, rope_rows, out_rows, window_nope, window_values, window_rope, key_up, value_up, allowed)
        current = lax.dynamic_slice_in_dim(carried, row_start, window_len, 0)
        carried = lax.dynamic_update_slice_in_dim(carried, current + partial_value, row_start, 0)
        return (carried, (grad_nope, grad_rope))
    carried, (grads_nope, grads_rope) = lax.scan(one_block, jnp.zeros((lead_rows + TOKENS, LATENT), jnp.float32), jnp.arange(N_CTX, dtype=jnp.int32))
    return (grads_nope.reshape(TOKENS, HEADS * NOPE), grads_rope.reshape(TOKENS, HEADS * ROPE), carried[lead_rows:])
```

```python
import functools
import math

import jax
import jax.numpy as jnp
from jax import lax
from jax.experimental import pallas as pl
from jax.experimental.pallas import tpu as pltpu
from jax.sharding import PartitionSpec as P

NOPE = 128
ROPE = 64
VDIM = 128
RANK = 512
STEPS = 3
BF = jnp.bfloat16
F32 = jnp.float32
MESH = pl.DeviceIdType.MESH
FOR_BACK, FOR_OWN, FROM_NEXT = 0, 1, 2


def dot_nt(a, b):
    return lax.dot_general(a, b, (((1,), (1,)), ((), ())), preferred_element_type=F32)


def dot_tn(a, b):
    return lax.dot_general(a, b, (((0,), (0,)), ((), ())), preferred_element_type=F32)


def kernel(
    n_ctx, n_head,
    keep_ref, lat_ref, qn_hbm, qr_hbm, go_hbm, ku_hbm, vu_hbm,
    dqn, dqr, dlat_ref,
    win, qn, qr, go, ku, vu, krlo, krhi, bias, keys, vals, dkeys, dvals, slopes_grad,
    rope_even, rope_odd, own, back, parts, got, zparts, zgot,
    load_sem, zs_sem, as_sem, bs_sem, cs_sem, win_sem,
    ps_sem, got_sem, ws_sem, zgot_sem,
):
    c = lax.axis_index("ctx")
    h = lax.axis_index("head")
    even = lax.rem(c, 2) == 0
    partner = jnp.where(even, c + 1, c - 1)
    far = jnp.where(even, c - 3, c + 3)
    has_far = (far >= 0) & (far < n_ctx)
    rows = lat_ref.shape[0]
    group = rows * n_head
    span = group * (STEPS + 1)
    heads = qn.shape[1] // NOPE
    scale = 1.0 / math.sqrt(NOPE + ROPE)

    loads = [
        pltpu.make_async_copy(src, dst, load_sem.at[i])
        for i, (src, dst) in enumerate(
            [(ku_hbm, ku), (vu_hbm, vu), (qn_hbm, qn), (qr_hbm, qr), (go_hbm, go)]
        )
    ]
    for load in loads:
        load.start()

    barrier = pltpu.get_barrier_semaphore()
    for t in range(1, n_head):
        pl.semaphore_signal(
            barrier, inc=1, device_id=(c, lax.rem(h + t, n_head)), device_id_type=MESH
        )
    pl.semaphore_signal(barrier, inc=1, device_id=(partner, h), device_id_type=MESH)
    for ok, who in ((c >= 2, c - 2), (c + 2 < n_ctx, c + 2), (has_far, far)):

        @pl.when(ok)
        def _():
            pl.semaphore_signal(barrier, inc=1, device_id=(who, h), device_id_type=MESH)

    peers = n_head
    for ok in (c >= 2, c + 2 < n_ctx, has_far):
        peers = peers + jnp.where(ok, 1, 0)
    pl.semaphore_wait(barrier, peers)

    def piece(t):
        return lax.rem(h - t + n_head, n_head)

    def over_head(t):
        return pltpu.make_async_remote_copy(
            src_ref=lat_ref, dst_ref=win.at[3, h], send_sem=zs_sem.at[t],
            recv_sem=win_sem.at[3, t], device_id=(c, lax.rem(h + t, n_head)),
            device_id_type=MESH,
        )

    def own_source(t):
        return lat_ref if t == 0 else win.at[3, piece(t)]

    def send_two_ahead(t):
        return pltpu.make_async_remote_copy(
            src_ref=own_source(t), dst_ref=win.at[1, piece(t)], send_sem=as_sem.at[t],
            recv_sem=win_sem.at[1, t], device_id=(c + 2, h), device_id_type=MESH,
        )

    b_slot = jnp.where(even, 2, 0)
    b_who = jnp.where(even, c + 1, c + 3)
    b_ok = b_who < n_ctx

    def send_odd_ahead(t):
        return pltpu.make_async_remote_copy(
            src_ref=own_source(t), dst_ref=win.at[b_slot, piece(t)], send_sem=bs_sem.at[t],
            recv_sem=win_sem.at[b_slot, t], device_id=(b_who, h), device_id_type=MESH,
        )

    c_slot = jnp.where(even, 0, 2)

    def forward(t):
        return pltpu.make_async_remote_copy(
            src_ref=win.at[1, piece(t)], dst_ref=win.at[c_slot, piece(t)], send_sem=cs_sem.at[t],
            recv_sem=win_sem.at[c_slot, t], device_id=(partner, h), device_id_type=MESH,
        )

    def wait_piece(slot, t):
        pltpu.make_async_remote_copy(
            src_ref=lat_ref, dst_ref=win.at[slot, piece(t)], send_sem=zs_sem.at[0],
            recv_sem=win_sem.at[slot, t], device_id=(partner, h), device_id_type=MESH,
        ).wait_recv()

    @pl.when(c + 2 < n_ctx)
    def _():
        send_two_ahead(0).start()

    for t in range(1, n_head):
        over_head(t).start()

    @pl.when(b_ok)
    def _():
        send_odd_ahead(0).start()

    own_copy = pltpu.make_async_copy(lat_ref, win.at[3, h], zs_sem.at[0])
    own_copy.start()

    key_at = lax.broadcasted_iota(jnp.int32, (group, group), 0)
    query_at = lax.broadcasted_iota(jnp.int32, (group, group), 1)
    bias[STEPS * group :, :] = jnp.where(key_at <= query_at, 0.0, -jnp.inf).astype(F32)
    for k in range(1, STEPS + 1):
        flag = jnp.where((keep_ref[0, k - 1] == 1) & (c >= k), 0.0, -jnp.inf).astype(F32)
        bias[(STEPS - k) * group : (STEPS - k + 1) * group, :] = jnp.full((group, group), flag, F32)

        @pl.when(c < k)
        def _():
            win[STEPS - k] = jnp.zeros(win.shape[1:], BF)

    rope_even[...] = jnp.zeros(rope_even.shape, F32)
    rope_odd[...] = jnp.zeros(rope_odd.shape, F32)

    for t in range(1, n_head):
        wait_piece(3, t)

        @pl.when(c + 2 < n_ctx)
        def _():
            send_two_ahead(t).start()

        @pl.when(b_ok)
        def _():
            send_odd_ahead(t).start()

    def at_pair(j, width):
        return pl.ds(pl.multiple_of(j * width, width), width)

    def expand(slots):
        size = len(slots) * group
        blocks = jnp.concatenate([win[i : i + 1] for i in slots], axis=0)
        content = blocks[:, :, :, :RANK].reshape(size, RANK)
        rope_keys = blocks[:, :, :, RANK:].reshape(size, ROPE)
        pad = jnp.zeros((size, ROPE), BF)
        low = jnp.concatenate([rope_keys, pad], axis=1)
        high = jnp.concatenate([pad, rope_keys], axis=1)

        def store(ref, lanes, value):
            for i, slot in enumerate(slots):
                ref[slot * group : (slot + 1) * group, lanes] = value[i * group : (i + 1) * group]

        store(krlo, slice(None), low)
        store(krhi, slice(None), high)

        def expand_step(j, carry):
            lanes = at_pair(j, 2 * NOPE)
            store(keys, lanes, jnp.dot(content, ku[:, lanes], preferred_element_type=F32).astype(BF))
            store(vals, lanes, jnp.dot(content, vu[:, lanes], preferred_element_type=F32).astype(BF))
            return carry

        lax.fori_loop(0, heads // 2, expand_step, 0, unroll=min(4, heads // 2))

    own_copy.wait()
    for load in loads:
        load.wait()
    expand((3,))

    @pl.when(c >= 2)
    def _():
        for t in range(n_head):
            wait_piece(1, t)
            forward(t).start()

    expand((1,))
    for k in (1, 3):

        @pl.when(c >= k)
        def _():
            for t in range(n_head):
                wait_piece(STEPS - k, t)

    expand((0, 2))

    def pair_step(j, carry):
        wide = at_pair(j, 2 * NOPE)
        key_pair = keys[:, wide]
        value_pair = vals[:, wide]
        qn_pair = qn[:, wide]
        go_pair = go[:, wide]
        qr_pair = qr[:, at_pair(j, 2 * ROPE)]
        dk, dv = [], []
        for e, (kr, rope_sum) in enumerate(((krlo, rope_even), (krhi, rope_odd))):
            lanes = slice(e * NOPE, (e + 1) * NOPE)
            key = jnp.concatenate([key_pair[:, lanes], kr[...]], axis=1)
            query = jnp.concatenate([qn_pair[:, lanes], qr_pair], axis=1)
            cotangent = go_pair[:, lanes]
            scores = dot_nt(key, query) * scale + bias[...]
            top = jnp.max(scores, axis=0, keepdims=True)
            exponent = jnp.exp(scores - top)
            probs = exponent * (1.0 / jnp.sum(exponent, axis=0, keepdims=True))
            weights = probs.astype(BF)
            slopes = dot_nt(value_pair[:, lanes], cotangent)
            delta = jnp.sum(weights.astype(F32) * slopes, axis=0, keepdims=True)
            score_grad = (probs * ((slopes - delta) * scale)).astype(BF)
            slopes_grad[2 * j + e] = score_grad
            both = jnp.dot(score_grad, query, preferred_element_type=F32)
            dk.append(both[:, :NOPE].astype(BF))
            rope_sum[...] += both[:, NOPE:]
            dv.append(jnp.dot(weights, cotangent, preferred_element_type=F32).astype(BF))
        dkeys[:, wide] = jnp.concatenate(dk, axis=1)
        dvals[:, wide] = jnp.concatenate(dv, axis=1)
        return carry

    lax.fori_loop(0, heads // 2, pair_step, 0, unroll=min(8, heads // 2))

    def terms_of(k):
        at = slice((STEPS - k) * group, (STEPS - k + 1) * group)
        content = dot_nt(dkeys[at, :], ku[...]) + dot_nt(dvals[at, :], vu[...])
        rope = rope_even[at, :ROPE] + rope_odd[at, ROPE:]
        return content.reshape(n_head, rows, RANK), rope.reshape(n_head, rows, ROPE)

    def put(ref, k):
        content, rope = terms_of(k)
        ref[:, :, :RANK] = content.astype(ref.dtype)
        ref[:, :, RANK:] = rope.astype(ref.dtype)

    order = [*range(1, n_head), 0]

    def chunk(t):
        return lax.rem(h + t, n_head)

    def send_part(i, slot, who, t):
        return pltpu.make_async_remote_copy(
            src_ref=parts.at[i, chunk(t)], dst_ref=got.at[slot, chunk(t)], send_sem=ps_sem.at[i, t],
            recv_sem=got_sem.at[slot, t], device_id=(who, h), device_id_type=MESH,
        )

    def part3(t):
        return send_part(0, jnp.where(even, FOR_OWN, FOR_BACK), jnp.where(even, c - 3, c - 1), t)

    def part1(t):
        return send_part(1, jnp.where(even, FOR_BACK, FOR_OWN), partner, t)

    def part2(t):
        return send_part(2, FROM_NEXT, c - 2, t)

    def wait_part(slot, t):
        send_part(0, slot, partner, t).wait_recv()

    put(parts.at[0], 3)

    @pl.when(c >= 3)
    def _():
        for t in order:
            part3(t).start()

    put(parts.at[1], 1)

    @pl.when(c >= 1)
    def _():
        for t in order:
            part1(t).start()

    put(back, 2)

    @pl.when(c >= 2)
    def _():
        for t in order:
            wait_part(FOR_BACK, t)
            parts[2, chunk(t)] = (back[chunk(t)] + got[FOR_BACK, chunk(t)].astype(F32)).astype(BF)
            part2(t).start()

    put(own, 0)

    def dq_step(j, carry):
        wide = at_pair(j, 2 * NOPE)
        key_pair = keys[:, wide]
        nope, rope = [], None
        for e, kr in enumerate((krlo, krhi)):
            key = jnp.concatenate([key_pair[:, e * NOPE : (e + 1) * NOPE], kr[...]], axis=1)
            both = dot_tn(slopes_grad[2 * j + e], key)
            nope.append(both[:, :NOPE])
            rope = both[:, NOPE:] if rope is None else rope + both[:, NOPE:]
        dqn[:, wide] = jnp.concatenate(nope, axis=1)
        dqr[:, at_pair(j, 2 * ROPE)] = rope
        return carry

    lax.fori_loop(0, heads // 2, dq_step, 0)
    own_ok = even | (c + 3 < n_ctx)

    def scatter(t):
        return pltpu.make_async_remote_copy(
            src_ref=zparts.at[chunk(t)], dst_ref=zgot.at[t], send_sem=ws_sem.at[t],
            recv_sem=zgot_sem.at[t], device_id=(c, chunk(t)), device_id_type=MESH,
        )

    for t in order:

        @pl.when(own_ok)
        def _():
            wait_part(FOR_OWN, t)
            own[chunk(t)] += got[FOR_OWN, chunk(t)].astype(F32)

        @pl.when(c + 2 < n_ctx)
        def _():
            wait_part(FROM_NEXT, t)
            own[chunk(t)] += got[FROM_NEXT, chunk(t)].astype(F32)

        if t > 0:
            zparts[chunk(t)] = own[chunk(t)].astype(BF)
            scatter(t).start()

    total = own[h]
    for t in range(1, n_head):
        scatter(t).wait_recv()
        total = total + zgot[t].astype(F32)
    dlat_ref[...] = total

    for t in range(1, n_head):
        scatter(t).wait_send()
        over_head(t).wait_send()

    @pl.when(c + 2 < n_ctx)
    def _():
        for t in range(n_head):
            send_two_ahead(t).wait_send()

    @pl.when(b_ok)
    def _():
        for t in range(n_head):
            send_odd_ahead(t).wait_send()

    @pl.when(c >= 2)
    def _():
        for t in range(n_head):
            forward(t).wait_send()
            part2(t).wait_send()

    @pl.when(c >= 1)
    def _():
        for t in range(n_head):
            part1(t).wait_send()

    @pl.when(c >= 3)
    def _():
        for t in range(n_head):
            part3(t).wait_send()


def write_out(a, b, c, a_hbm, b_hbm, c_hbm, sem):
    copies = [
        pltpu.make_async_copy(src, dst, sem.at[i])
        for i, (src, dst) in enumerate([(a, a_hbm), (b, b_hbm), (c, c_hbm)])
    ]
    for copy in copies:
        copy.start()
    for copy in copies:
        copy.wait()


def on_device(n_ctx, n_head, query_nope, query_rope, grad_out, latent, key_up, value_up, block_keep):
    rows, width = latent.shape
    group = query_nope.shape[0]
    span = group * (STEPS + 1)
    wide = query_nope.shape[1]
    rope_wide = query_rope.shape[1]
    heads = wide // NOPE
    assert block_keep.shape[1] == STEPS and n_ctx % 2 == 0
    vmem, hbm = pl.BlockSpec(memory_space=pltpu.VMEM), pl.BlockSpec(memory_space=pl.ANY)
    dma = pltpu.SemaphoreType.DMA
    block = (n_head, rows, width)
    results = pl.pallas_call(
        functools.partial(kernel, n_ctx, n_head),
        out_shape=(
            pltpu.VMEM((group, wide), F32),
            pltpu.VMEM((group, rope_wide), F32),
            pltpu.VMEM((rows, width), F32),
        ),
        in_specs=[pl.BlockSpec(memory_space=pltpu.SMEM), vmem, hbm, hbm, hbm, hbm, hbm],
        out_specs=(vmem, vmem, vmem),
        scratch_shapes=[
            pltpu.VMEM((STEPS + 1,) + block, BF),
            pltpu.VMEM((group, wide), BF),
            pltpu.VMEM((group, rope_wide), BF),
            pltpu.VMEM((group, wide), BF),
            pltpu.VMEM((RANK, wide), BF),
            pltpu.VMEM((RANK, wide), BF),
            pltpu.VMEM((span, 2 * ROPE), BF),
            pltpu.VMEM((span, 2 * ROPE), BF),
            pltpu.VMEM((span, group), F32),
            pltpu.VMEM((span, wide), BF),
            pltpu.VMEM((span, wide), BF),
            pltpu.VMEM((span, wide), BF),
            pltpu.VMEM((span, wide), BF),
            pltpu.VMEM((heads, span, group), BF),
            pltpu.VMEM((span, 2 * ROPE), F32),
            pltpu.VMEM((span, 2 * ROPE), F32),
            pltpu.VMEM(block, F32),
            pltpu.VMEM(block, F32),
            pltpu.VMEM((3,) + block, BF),
            pltpu.VMEM((3,) + block, BF),
            pltpu.VMEM(block, BF),
            pltpu.VMEM(block, BF),
            dma((5,)),
            dma((n_head,)),
            dma((n_head,)),
            dma((n_head,)),
            dma((n_head,)),
            dma((STEPS + 1, n_head)),
            dma((3, n_head)),
            dma((3, n_head)),
            dma((n_head,)),
            dma((n_head,)),
        ],
        compiler_params=pltpu.CompilerParams(collective_id=0, has_side_effects=True),
        name="latent_attention_grads",
    )(block_keep, latent, query_nope, query_rope, grad_out, key_up, value_up)

    return pl.pallas_call(
        write_out,
        out_shape=tuple(jax.ShapeDtypeStruct(r.shape, r.dtype) for r in results),
        in_specs=[vmem] * 3,
        out_specs=[hbm] * 3,
        scratch_shapes=[dma((3,))],
        name="write_out",
    )(*(pltpu.with_memory_space_constraint(r, pltpu.VMEM) for r in results))


def solution(mesh):
    placed = (
        P("ctx", "head"),
        P("ctx", "head"),
        P("ctx", "head"),
        P(("ctx", "head"), None),
        P(None, "head"),
        P(None, "head"),
        P("ctx", None),
    )
    return jax.shard_map(
        functools.partial(on_device, mesh.shape["ctx"], mesh.shape["head"]),
        mesh=mesh,
        in_specs=placed,
        out_specs=(P("ctx", "head"), P("ctx", "head"), P(("ctx", "head"), None)),
        check_vma=False,
    )
```

```python
import functools
import math

import jax
import jax.numpy as jnp
from jax import lax
from jax.experimental import pallas as pl
from jax.experimental.pallas import tpu as pltpu
from jax.sharding import PartitionSpec as P

NOPE = 128
ROPE = 64
VDIM = 128
RANK = 512
STEPS = 3
BF = jnp.bfloat16
F32 = jnp.float32
MESH = pl.DeviceIdType.MESH
FOR_BACK, FOR_OWN, FROM_NEXT = 0, 1, 2


def dot_nt(a, b):
    return lax.dot_general(a, b, (((1,), (1,)), ((), ())), preferred_element_type=F32)


def dot_tn(a, b):
    return lax.dot_general(a, b, (((0,), (0,)), ((), ())), preferred_element_type=F32)


def two_heads(pair):
    width = pair.shape[1] // 2
    zero = jnp.zeros((pair.shape[0], width), pair.dtype)
    first = jnp.concatenate([pair[:, :width], zero], axis=1)
    second = jnp.concatenate([zero, pair[:, width:]], axis=1)
    return jnp.concatenate([first, second], axis=0)


def kernel(
    n_ctx, n_head,
    keep_hbm, lat_hbm, qn_hbm, qr_hbm, go_hbm, ku_hbm, vu_hbm,
    dqn, dqr, dlat_ref,
    keep, win, qn, qr, go, ku, vu, kut, vut, qrs, krlo, krhi, bias, keys, vals, dkeys, dvals, slopes_grad,
    raw, tops, slopes, weights, own, back, parts, got, zparts, zgot,
    load_sem, lat_sem, keep_sem, zs_sem, as_sem, bs_sem, cs_sem, win_sem,
    ps_sem, got_sem, ws_sem, zgot_sem,
):
    c = lax.axis_index("ctx")
    h = lax.axis_index("head")
    even = lax.rem(c, 2) == 0
    partner = jnp.where(even, c + 1, c - 1)
    far = jnp.where(even, c - 3, c + 3)
    has_far = (far >= 0) & (far < n_ctx)
    rows = lat_hbm.shape[0]
    group = rows * n_head
    span = group * (STEPS + 1)
    heads = qn.shape[1] // NOPE
    scale = 1.0 / math.sqrt(NOPE + ROPE)

    loads = [
        pltpu.make_async_copy(src, dst, load_sem.at[i])
        for i, (src, dst) in enumerate(
            [(ku_hbm, ku), (vu_hbm, vu), (qn_hbm, qn), (qr_hbm, qr), (go_hbm, go)]
        )
    ]
    barrier = pltpu.get_barrier_semaphore()
    for t in range(1, n_head):
        pl.semaphore_signal(
            barrier, inc=1, device_id=(c, lax.rem(h + t, n_head)), device_id_type=MESH
        )
    pl.semaphore_signal(barrier, inc=1, device_id=(partner, h), device_id_type=MESH)
    for ok, who in ((c >= 2, c - 2), (c + 2 < n_ctx, c + 2), (has_far, far)):

        @pl.when(ok)
        def _():
            pl.semaphore_signal(barrier, inc=1, device_id=(who, h), device_id_type=MESH)

    own_copy = pltpu.make_async_copy(lat_hbm, win.at[3, h], lat_sem)
    own_copy.start()
    keep_copy = pltpu.make_async_copy(keep_hbm, keep, keep_sem)
    keep_copy.start()
    for load in loads:
        load.start()

    peers = n_head
    for ok in (c >= 2, c + 2 < n_ctx, has_far):
        peers = peers + jnp.where(ok, 1, 0)
    key_at = lax.broadcasted_iota(jnp.int32, (group, group), 0)
    query_at = lax.broadcasted_iota(jnp.int32, (group, group), 1)
    bias[...] = jnp.where(key_at <= query_at, 0.0, -jnp.inf).astype(F32)
    keep_copy.wait()
    flags = [None] * STEPS
    for k in range(1, STEPS + 1):
        flags[STEPS - k] = jnp.where((keep[0, k - 1] == 1) & (c >= k), 0.0, -jnp.inf).astype(F32)

        @pl.when(c < k)
        def _():
            win[STEPS - k] = jnp.zeros(win.shape[1:], BF)

    def at_pair(j, width):
        return pl.ds(pl.multiple_of(j * width, width), width)

    def transpose(src, dst):
        def step(j, carry):
            dst[at_pair(j, 2 * NOPE), :] = src[:, at_pair(j, 2 * NOPE)].T
            return carry

        lax.fori_loop(0, heads // 2, step, 0, unroll=2)

    loads[0].wait()
    transpose(ku, kut)
    pl.semaphore_wait(barrier, peers)
    own_copy.wait()

    before, after = h, n_head - 1 - h
    twice = 2 * jnp.minimum(before, after)

    def near(t):
        if t == 0:
            return h
        both = h - (t + 1) // 2 if t % 2 else h + t // 2
        rest = t - jnp.minimum(before, after)
        return jnp.where(t <= twice, both, jnp.where(before < after, h + rest, h - rest))

    piece = near

    def over_head(t):
        return pltpu.make_async_remote_copy(
            src_ref=win.at[3, h], dst_ref=win.at[3, h], send_sem=zs_sem.at[t],
            recv_sem=win_sem.at[3, h], device_id=(c, near(t)), device_id_type=MESH,
        )

    def own_source(t):
        return win.at[3, piece(t)]

    def send_two_ahead(t):
        return pltpu.make_async_remote_copy(
            src_ref=own_source(t), dst_ref=win.at[1, piece(t)], send_sem=as_sem.at[t],
            recv_sem=win_sem.at[1, piece(t)], device_id=(c + 2, h), device_id_type=MESH,
        )

    b_slot = jnp.where(even, 2, 0)
    b_who = jnp.where(even, c + 1, c + 3)
    b_ok = b_who < n_ctx

    def send_odd_ahead(t):
        return pltpu.make_async_remote_copy(
            src_ref=own_source(t), dst_ref=win.at[b_slot, piece(t)], send_sem=bs_sem.at[t],
            recv_sem=win_sem.at[b_slot, piece(t)], device_id=(b_who, h), device_id_type=MESH,
        )

    c_slot = jnp.where(even, 0, 2)

    def forward(t):
        return pltpu.make_async_remote_copy(
            src_ref=win.at[1, piece(t)], dst_ref=win.at[c_slot, piece(t)], send_sem=cs_sem.at[t],
            recv_sem=win_sem.at[c_slot, piece(t)], device_id=(partner, h), device_id_type=MESH,
        )

    def wait_piece(slot, t):
        pltpu.make_async_remote_copy(
            src_ref=win.at[3, h], dst_ref=win.at[slot, piece(t)], send_sem=zs_sem.at[0],
            recv_sem=win_sem.at[slot, piece(t)], device_id=(partner, h), device_id_type=MESH,
        ).wait_recv()

    @pl.when(c + 2 < n_ctx)
    def _():
        send_two_ahead(0).start()

    for t in range(1, n_head):
        over_head(n_head - t).start()

    @pl.when(b_ok)
    def _():
        send_odd_ahead(0).start()

    for load in loads[1:]:
        load.wait()
    transpose(vu, vut)

    low_half = lax.broadcasted_iota(jnp.int32, (group, 2 * ROPE), 1) < ROPE

    def stack_step(j, carry):
        pair = qr[:, at_pair(j, 2 * ROPE)]
        for e, mine in enumerate((low_half, jnp.logical_not(low_half))):
            at = pl.ds(pl.multiple_of((2 * j + e) * group, group), group)
            qrs[at, :] = jnp.where(mine, pair, jnp.zeros_like(pair))
        return carry

    lax.fori_loop(0, heads // 2, stack_step, 0, unroll=2)

    for t in range(1, n_head):
        wait_piece(3, t)

        @pl.when(c + 2 < n_ctx)
        def _():
            send_two_ahead(t).start()

        @pl.when(b_ok)
        def _():
            send_odd_ahead(t).start()

    def expand(slot):
        content = win[slot, :, :, :RANK].reshape(group, RANK)
        rope_keys = win[slot, :, :, RANK:].reshape(group, ROPE)
        pad = jnp.zeros((group, ROPE), BF)
        at = pl.ds(pl.multiple_of(slot * group, group), group)
        krlo[at, :] = jnp.concatenate([rope_keys, pad], axis=1)
        krhi[at, :] = jnp.concatenate([pad, rope_keys], axis=1)

        def expand_step(j, carry):
            lanes = at_pair(j, 2 * NOPE)
            keys[at, lanes] = jnp.dot(content, ku[:, lanes], preferred_element_type=F32).astype(BF)
            vals[at, lanes] = jnp.dot(content, vu[:, lanes], preferred_element_type=F32).astype(BF)
            return carry

        lax.fori_loop(0, heads // 2, expand_step, 0, unroll=heads // 2)

    def take(slot, passing_on=False):
        @pl.when(c >= STEPS - slot)
        def _():
            for t in range(n_head):
                wait_piece(slot, t)
                if passing_on:
                    forward(t).start()

        expand(slot)

    expand(STEPS)
    take(jnp.where(even, 0, 2))
    take(1, True)
    take(jnp.where(even, 2, 0))

    pairs = heads // 2
    rate = scale * math.log2(math.e)
    blocks = [slice(i * group, (i + 1) * group) for i in range(STEPS + 1)]

    def fold(value, how):
        return how(value.reshape(group // 8, 8, group), axis=0)

    def lanes_of(e):
        return slice(e * NOPE, (e + 1) * NOPE)

    def score_pair(j, at):
        wide = at_pair(j, 2 * NOPE)
        key_pair = keys[:, wide]
        qn_pair = qn[:, wide]
        qr_pair = qr[:, at_pair(j, 2 * ROPE)]
        for e, kr in enumerate((krlo, krhi)):
            key = jnp.concatenate([key_pair[:, lanes_of(e)], kr[...]], axis=1)
            query = jnp.concatenate([qn_pair[:, lanes_of(e)], qr_pair], axis=1)
            scores = dot_nt(key, query)
            top = None
            for i, block in enumerate(blocks):
                piece = scores[block]
                if i == STEPS:
                    piece = piece + bias[...]
                raw[at, block, lanes_of(e)] = piece
                high = fold(piece, jnp.max)
                if i < STEPS:
                    high = high + flags[i]
                top = high if top is None else jnp.maximum(top, high)
            tops[at, :, lanes_of(e)] = jnp.broadcast_to(jnp.max(top, axis=0, keepdims=True), (8, group))
        slopes[at] = dot_nt(vals[:, wide], two_heads(go[:, wide]))

    def softmax_pair(j, at):
        for e in range(2):
            lanes = lanes_of(e)
            top = tops[at, 0:1, lanes] * rate
            shift = [top - flags[i] if i < STEPS else top for i in range(STEPS + 1)]
            total = None
            for i, block in enumerate(blocks):
                part = fold(jnp.exp2(raw[at, block, lanes] * rate - shift[i]), jnp.sum)
                total = part if total is None else total + part
            norm = jnp.log2(jnp.sum(total, axis=0, keepdims=True))
            delta = None
            for i, block in enumerate(blocks):
                probs = jnp.exp2(raw[at, block, lanes] * rate - (shift[i] + norm))
                weights[at, block, lanes] = probs.astype(BF)
                part = fold(probs * slopes[at, block, lanes], jnp.sum)
                delta = part if delta is None else delta + part
            delta = jnp.sum(delta, axis=0, keepdims=True)
            mine = at_pair(2 * j + e, group)
            for block in blocks:
                slope = ((slopes[at, block, lanes] - delta) * scale).astype(BF)
                slopes_grad[block, mine] = weights[at, block, lanes] * slope

    def grad_pair(j, at):
        wide = at_pair(j, 2 * NOPE)
        grad = slopes_grad[:, at_pair(j, 2 * group)]
        dkeys[:, wide] = jnp.dot(grad, two_heads(qn[:, wide]), preferred_element_type=F32).astype(BF)
        dvals[:, wide] = jnp.dot(weights[at], two_heads(go[:, wide]), preferred_element_type=F32).astype(BF)

    score_pair(0, 0)
    score_pair(1, 1)
    softmax_pair(0, 0)

    def pair_step(j, carry):
        now = lax.rem(j, 2)
        grad_pair(j - 1, 1 - now)
        score_pair(j + 1, 1 - now)
        softmax_pair(j, now)
        return carry

    lax.fori_loop(1, pairs - 1, pair_step, 0, unroll=min(6, pairs - 2))
    last = (pairs - 1) % 2
    grad_pair(pairs - 2, 1 - last)
    softmax_pair(pairs - 1, last)
    grad_pair(pairs - 1, last)

    def terms_of(k):
        at = pl.ds(pl.multiple_of((STEPS - k) * group, group), group)
        content = jnp.dot(dkeys[at, :], kut[...], preferred_element_type=F32)
        content = content + jnp.dot(dvals[at, :], vut[...], preferred_element_type=F32)
        both = jnp.dot(slopes_grad[at, :], qrs[...], preferred_element_type=F32)
        rope = both[:, :ROPE] + both[:, ROPE:]
        return content.reshape(n_head, rows, RANK), rope.reshape(n_head, rows, ROPE)

    def put(ref, k):
        content, rope = terms_of(k)
        ref[:, :, :RANK] = content.astype(ref.dtype)
        ref[:, :, RANK:] = rope.astype(ref.dtype)

    order = [*range(n_head - 1, 0, -1), 0]
    chunk = near
    back_k, own_k = jnp.where(even, 1, 3), jnp.where(even, 3, 1)
    far_who = jnp.where(even, c - 3, c - 1)

    def send_part(i, slot, who, t):
        return pltpu.make_async_remote_copy(
            src_ref=parts.at[i, chunk(t)], dst_ref=got.at[slot, chunk(t)], send_sem=ps_sem.at[i, t],
            recv_sem=got_sem.at[slot, chunk(t)], device_id=(who, h), device_id_type=MESH,
        )

    def part_back(t):
        return send_part(0, FOR_BACK, partner, t)

    def part_next(t):
        return send_part(2, FROM_NEXT, c - 2, t)

    def part_own(t):
        return send_part(1, FOR_OWN, far_who, t)

    def wait_part(slot, t):
        send_part(0, slot, partner, t).wait_recv()

    def put_own_part():
        put(parts.at[1], own_k)

        @pl.when(c >= own_k)
        def _():
            for t in order:
                part_own(t).start()

    own_first = (lax.rem(c, 4) == 2) & (c >= own_k)
    pl.when(own_first)(put_own_part)

    put(parts.at[0], back_k)

    @pl.when(c >= back_k)
    def _():
        for t in order:
            part_back(t).start()

    put(back, 2)

    @pl.when(c >= 2)
    def _():
        for t in order:
            wait_part(FOR_BACK, t)
            parts[2, chunk(t)] = (back[chunk(t)] + got[FOR_BACK, chunk(t)].astype(F32)).astype(BF)
            part_next(t).start()

    pl.when(jnp.logical_not(own_first))(put_own_part)

    put(own, 0)

    def dq_step(j, carry):
        wide = at_pair(j, 2 * NOPE)
        key_pair = keys[:, wide]
        nope, rope = [], None
        for e, kr in enumerate((krlo, krhi)):
            key = jnp.concatenate([key_pair[:, e * NOPE : (e + 1) * NOPE], kr[...]], axis=1)
            both = dot_tn(slopes_grad[:, at_pair(2 * j + e, group)], key)
            nope.append(both[:, :NOPE])
            rope = both[:, NOPE:] if rope is None else rope + both[:, NOPE:]
        dqn[:, wide] = jnp.concatenate(nope, axis=1)
        dqr[:, at_pair(j, 2 * ROPE)] = rope
        return carry

    lax.fori_loop(0, heads // 2, dq_step, 0, unroll=2)
    own_ok = even | (c + 3 < n_ctx)

    def scatter(t):
        return pltpu.make_async_remote_copy(
            src_ref=zparts.at[chunk(t)], dst_ref=zgot.at[h], send_sem=ws_sem.at[t],
            recv_sem=zgot_sem.at[h], device_id=(c, chunk(t)), device_id_type=MESH,
        )

    for t in order:

        @pl.when(own_ok)
        def _():
            wait_part(FOR_OWN, t)
            own[chunk(t)] += got[FOR_OWN, chunk(t)].astype(F32)

        @pl.when(c + 2 < n_ctx)
        def _():
            wait_part(FROM_NEXT, t)
            own[chunk(t)] += got[FROM_NEXT, chunk(t)].astype(F32)

        if t > 0:
            zparts[chunk(t)] = own[chunk(t)].astype(BF)
            scatter(t).start()

    total = own[h]
    for t in range(1, n_head):
        pltpu.make_async_remote_copy(
            src_ref=zparts.at[h], dst_ref=zgot.at[near(t)], send_sem=ws_sem.at[t],
            recv_sem=zgot_sem.at[near(t)], device_id=(c, near(t)), device_id_type=MESH,
        ).wait_recv()
        total = total + zgot[near(t)].astype(F32)
    dlat_ref[...] = total

    for t in range(1, n_head):
        scatter(t).wait_send()
        over_head(t).wait_send()

    @pl.when(c + 2 < n_ctx)
    def _():
        for t in range(n_head):
            send_two_ahead(t).wait_send()

    @pl.when(b_ok)
    def _():
        for t in range(n_head):
            send_odd_ahead(t).wait_send()

    @pl.when(c >= 2)
    def _():
        for t in range(n_head):
            forward(t).wait_send()
            part_next(t).wait_send()

    @pl.when(c >= back_k)
    def _():
        for t in range(n_head):
            part_back(t).wait_send()

    @pl.when(c >= own_k)
    def _():
        for t in range(n_head):
            part_own(t).wait_send()


def write_out(a, b, c, a_hbm, b_hbm, c_hbm, sem):
    copies = [
        pltpu.make_async_copy(src, dst, sem.at[i])
        for i, (src, dst) in enumerate([(a, a_hbm), (b, b_hbm), (c, c_hbm)])
    ]
    for copy in copies:
        copy.start()
    for copy in copies:
        copy.wait()


def on_device(n_ctx, n_head, query_nope, query_rope, grad_out, latent, key_up, value_up, block_keep):
    rows, width = latent.shape
    group = query_nope.shape[0]
    span = group * (STEPS + 1)
    wide = query_nope.shape[1]
    rope_wide = query_rope.shape[1]
    heads = wide // NOPE
    assert block_keep.shape[1] == STEPS and n_ctx % 2 == 0 and heads % 2 == 0 and heads >= 4
    vmem, hbm = pl.BlockSpec(memory_space=pltpu.VMEM), pl.BlockSpec(memory_space=pl.ANY)
    dma = pltpu.SemaphoreType.DMA
    block = (n_head, rows, width)
    results = pl.pallas_call(
        functools.partial(kernel, n_ctx, n_head),
        out_shape=(
            pltpu.VMEM((group, wide), F32),
            pltpu.VMEM((group, rope_wide), F32),
            pltpu.VMEM((rows, width), F32),
        ),
        in_specs=[hbm, hbm, hbm, hbm, hbm, hbm, hbm],
        out_specs=(vmem, vmem, vmem),
        scratch_shapes=[
            pltpu.SMEM(block_keep.shape, block_keep.dtype),
            pltpu.VMEM((STEPS + 1,) + block, BF),
            pltpu.VMEM((group, wide), BF),
            pltpu.VMEM((group, rope_wide), BF),
            pltpu.VMEM((group, wide), BF),
            pltpu.VMEM((RANK, wide), BF),
            pltpu.VMEM((RANK, wide), BF),
            pltpu.VMEM((wide, RANK), BF),
            pltpu.VMEM((wide, RANK), BF),
            pltpu.VMEM((heads * group, 2 * ROPE), BF),
            pltpu.VMEM((span, 2 * ROPE), BF),
            pltpu.VMEM((span, 2 * ROPE), BF),
            pltpu.VMEM((group, group), F32),
            pltpu.VMEM((span, wide), BF),
            pltpu.VMEM((span, wide), BF),
            pltpu.VMEM((span, wide), BF),
            pltpu.VMEM((span, wide), BF),
            pltpu.VMEM((span, heads * group), BF),
            pltpu.VMEM((2, span, 2 * group), F32),
            pltpu.VMEM((2, 8, 2 * group), F32),
            pltpu.VMEM((2, span, 2 * group), F32),
            pltpu.VMEM((2, span, 2 * group), BF),
            pltpu.VMEM(block, F32),
            pltpu.VMEM(block, F32),
            pltpu.VMEM((3,) + block, BF),
            pltpu.VMEM((3,) + block, BF),
            pltpu.VMEM(block, BF),
            pltpu.VMEM(block, BF),
            dma((5,)),
            dma(()),
            dma(()),
            dma((n_head,)),
            dma((n_head,)),
            dma((n_head,)),
            dma((n_head,)),
            dma((STEPS + 1, n_head)),
            dma((3, n_head)),
            dma((3, n_head)),
            dma((n_head,)),
            dma((n_head,)),
        ],
        compiler_params=pltpu.CompilerParams(collective_id=0, has_side_effects=True),
        name="latent_attention_grads",
    )(block_keep, latent, query_nope, query_rope, grad_out, key_up, value_up)

    return pl.pallas_call(
        write_out,
        out_shape=tuple(jax.ShapeDtypeStruct(r.shape, r.dtype) for r in results),
        in_specs=[vmem] * 3,
        out_specs=[hbm] * 3,
        scratch_shapes=[dma((3,))],
        name="write_out",
    )(*(pltpu.with_memory_space_constraint(r, pltpu.VMEM) for r in results))


def solution(mesh):
    placed = (
        P("ctx", "head"),
        P("ctx", "head"),
        P("ctx", "head"),
        P(("ctx", "head"), None),
        P(None, "head"),
        P(None, "head"),
        P("ctx", None),
    )
    return jax.shard_map(
        functools.partial(on_device, mesh.shape["ctx"], mesh.shape["head"]),
        mesh=mesh,
        in_specs=placed,
        out_specs=(P("ctx", "head"), P("ctx", "head"), P(("ctx", "head"), None)),
        check_vma=False,
    )
```

```python
import functools
import math

import jax
import jax.numpy as jnp
from jax import lax
from jax.experimental import pallas as pl
from jax.experimental.pallas import tpu as pltpu
from jax.sharding import PartitionSpec as P

NOPE = 128
ROPE = 64
VDIM = 128
RANK = 512
STEPS = 3
BF = jnp.bfloat16
F32 = jnp.float32
MESH = pl.DeviceIdType.MESH
FOR_BACK, FOR_OWN, FROM_NEXT = 0, 1, 2


def dot_nt(a, b):
    return lax.dot_general(a, b, (((1,), (1,)), ((), ())), preferred_element_type=F32)


def dot_tn(a, b):
    return lax.dot_general(a, b, (((0,), (0,)), ((), ())), preferred_element_type=F32)


def two_heads(pair):
    width = pair.shape[1] // 2
    zero = jnp.zeros((pair.shape[0], width), pair.dtype)
    first = jnp.concatenate([pair[:, :width], zero], axis=1)
    second = jnp.concatenate([zero, pair[:, width:]], axis=1)
    return jnp.concatenate([first, second], axis=0)


def kernel(
    n_ctx, n_head,
    keep_hbm, lat_hbm, qn_hbm, qr_hbm, go_hbm, ku_hbm, vu_hbm,
    dqn, dqr, dlat_ref,
    keep, win, qn, qr, go, ku, vu, kut, vut, qrs, krlo, krhi, bias, keys, vals, dkeys, dvals, slopes_grad,
    raw, tops, slopes, weights, own, back, parts, got, zparts, zgot,
    load_sem, lat_sem, keep_sem, zs_sem, as_sem, bs_sem, cs_sem, ds_sem, win_sem,
    ps_sem, got_sem, ws_sem, zgot_sem,
):
    c = lax.axis_index("ctx")
    h = lax.axis_index("head")
    even = lax.rem(c, 2) == 0
    partner = jnp.where(even, c + 1, c - 1)
    rows = lat_hbm.shape[0]
    group = rows * n_head
    span = group * (STEPS + 1)
    heads = qn.shape[1] // NOPE
    scale = 1.0 / math.sqrt(NOPE + ROPE)

    loads = [
        pltpu.make_async_copy(src, dst, load_sem.at[i])
        for i, (src, dst) in enumerate(
            [(ku_hbm, ku), (vu_hbm, vu), (qn_hbm, qn), (qr_hbm, qr), (go_hbm, go)]
        )
    ]
    barrier = pltpu.get_barrier_semaphore()
    for t in range(1, n_head):
        pl.semaphore_signal(
            barrier, inc=1, device_id=(c, lax.rem(h + t, n_head)), device_id_type=MESH
        )
    pl.semaphore_signal(barrier, inc=1, device_id=(partner, h), device_id_type=MESH)
    for ok, who in ((c >= 2, c - 2), (c + 2 < n_ctx, c + 2), (c >= 3, c - 3), (c + 3 < n_ctx, c + 3)):

        @pl.when(ok)
        def _():
            pl.semaphore_signal(barrier, inc=1, device_id=(who, h), device_id_type=MESH)

    own_copy = pltpu.make_async_copy(lat_hbm, win.at[3, h], lat_sem)
    own_copy.start()
    keep_copy = pltpu.make_async_copy(keep_hbm, keep, keep_sem)
    keep_copy.start()
    for load in loads:
        load.start()

    peers = n_head
    for ok in (c >= 2, c + 2 < n_ctx, c >= 3, c + 3 < n_ctx):
        peers = peers + jnp.where(ok, 1, 0)
    key_at = lax.broadcasted_iota(jnp.int32, (group, group), 0)
    query_at = lax.broadcasted_iota(jnp.int32, (group, group), 1)
    bias[...] = jnp.where(key_at <= query_at, 0.0, -jnp.inf).astype(F32)
    keep_copy.wait()
    flags = [None] * STEPS
    for k in range(1, STEPS + 1):
        flags[STEPS - k] = jnp.where((keep[0, k - 1] == 1) & (c >= k), 0.0, -jnp.inf).astype(F32)

        @pl.when(c < k)
        def _():
            win[STEPS - k] = jnp.zeros(win.shape[1:], BF)

    def at_pair(j, width):
        return pl.ds(pl.multiple_of(j * width, width), width)

    def transpose(src, dst):
        def step(j, carry):
            dst[at_pair(j, 2 * NOPE), :] = src[:, at_pair(j, 2 * NOPE)].T
            return carry

        lax.fori_loop(0, heads // 2, step, 0, unroll=2)

    loads[0].wait()
    transpose(ku, kut)
    pl.semaphore_wait(barrier, peers)
    own_copy.wait()

    before, after = h, n_head - 1 - h
    twice = 2 * jnp.minimum(before, after)

    def near(t):
        if t == 0:
            return h
        both = h - (t + 1) // 2 if t % 2 else h + t // 2
        rest = t - jnp.minimum(before, after)
        return jnp.where(t <= twice, both, jnp.where(before < after, h + rest, h - rest))

    piece = near

    def over_head(t):
        return pltpu.make_async_remote_copy(
            src_ref=win.at[3, h], dst_ref=win.at[3, h], send_sem=zs_sem,
            recv_sem=win_sem.at[3, h], device_id=(c, near(t)), device_id_type=MESH,
        )

    def own_source(t):
        return win.at[3, piece(t)]

    def send_two_ahead(t):
        return pltpu.make_async_remote_copy(
            src_ref=own_source(t), dst_ref=win.at[1, piece(t)], send_sem=as_sem,
            recv_sem=win_sem.at[1, piece(t)], device_id=(c + 2, h), device_id_type=MESH,
        )

    b_slot = jnp.where(even, 2, 0)
    b_who = jnp.where(even, c + 1, c + 3)
    b_ok = b_who < n_ctx

    def send_odd_ahead(t):
        return pltpu.make_async_remote_copy(
            src_ref=own_source(t), dst_ref=win.at[b_slot, piece(t)], send_sem=bs_sem,
            recv_sem=win_sem.at[b_slot, piece(t)], device_id=(b_who, h), device_id_type=MESH,
        )

    c_slot = jnp.where(even, 0, 2)

    late = n_head // 2
    direct_ok = even & (c + 3 < n_ctx)

    def send_direct(t):
        return pltpu.make_async_remote_copy(
            src_ref=own_source(t), dst_ref=win.at[0, piece(t)], send_sem=ds_sem,
            recv_sem=win_sem.at[0, piece(t)], device_id=(c + 3, h), device_id_type=MESH,
        )

    def forward(t):
        return pltpu.make_async_remote_copy(
            src_ref=win.at[1, piece(t)], dst_ref=win.at[c_slot, piece(t)], send_sem=cs_sem,
            recv_sem=win_sem.at[c_slot, piece(t)], device_id=(partner, h), device_id_type=MESH,
        )

    def wait_piece(slot, t):
        pltpu.make_async_remote_copy(
            src_ref=win.at[3, h], dst_ref=win.at[slot, piece(t)], send_sem=zs_sem,
            recv_sem=win_sem.at[slot, piece(t)], device_id=(partner, h), device_id_type=MESH,
        ).wait_recv()

    @pl.when(c + 2 < n_ctx)
    def _():
        send_two_ahead(0).start()

    for t in range(1, n_head):
        over_head(n_head - t).start()

    @pl.when(b_ok)
    def _():
        send_odd_ahead(0).start()

    for load in loads[1:]:
        load.wait()
    transpose(vu, vut)

    low_half = lax.broadcasted_iota(jnp.int32, (group, 2 * ROPE), 1) < ROPE

    def stack_step(j, carry):
        pair = qr[:, at_pair(j, 2 * ROPE)]
        for e, mine in enumerate((low_half, jnp.logical_not(low_half))):
            at = pl.ds(pl.multiple_of((2 * j + e) * group, group), group)
            qrs[at, :] = jnp.where(mine, pair, jnp.zeros_like(pair))
        return carry

    lax.fori_loop(0, heads // 2, stack_step, 0, unroll=2)

    for t in range(1, n_head):
        wait_piece(3, t)

        @pl.when(c + 2 < n_ctx)
        def _():
            send_two_ahead(t).start()

        if t >= late:

            @pl.when(direct_ok)
            def _():
                send_direct(t).start()

        @pl.when(b_ok)
        def _():
            send_odd_ahead(t).start()

    def expand(slot):
        content = win[slot, :, :, :RANK].reshape(group, RANK)
        rope_keys = win[slot, :, :, RANK:].reshape(group, ROPE)
        pad = jnp.zeros((group, ROPE), BF)
        at = pl.ds(pl.multiple_of(slot * group, group), group)
        krlo[at, :] = jnp.concatenate([rope_keys, pad], axis=1)
        krhi[at, :] = jnp.concatenate([pad, rope_keys], axis=1)

        def expand_step(j, carry):
            lanes = at_pair(j, 2 * NOPE)
            keys[at, lanes] = jnp.dot(content, ku[:, lanes], preferred_element_type=F32).astype(BF)
            vals[at, lanes] = jnp.dot(content, vu[:, lanes], preferred_element_type=F32).astype(BF)
            return carry

        lax.fori_loop(0, heads // 2, expand_step, 0, unroll=heads // 2)

    def take(slot, passing_on=False):
        @pl.when(c >= STEPS - slot)
        def _():
            for t in range(n_head):
                wait_piece(slot, t)
                if passing_on and t < late:
                    forward(t).start()
                elif passing_on:

                    @pl.when(jnp.logical_not(even))
                    def _():
                        forward(t).start()

        expand(slot)

    expand(STEPS)
    take(jnp.where(even, 0, 2))
    take(1, True)
    take(jnp.where(even, 2, 0))

    pairs = heads // 2
    rate = scale * math.log2(math.e)
    blocks = [slice(i * group, (i + 1) * group) for i in range(STEPS + 1)]

    def fold(value, how):
        return how(value.reshape(group // 8, 8, group), axis=0)

    def lanes_of(e):
        return slice(e * NOPE, (e + 1) * NOPE)

    def score_pair(j, at):
        wide = at_pair(j, 2 * NOPE)
        key_pair = keys[:, wide]
        qn_pair = qn[:, wide]
        qr_pair = qr[:, at_pair(j, 2 * ROPE)]
        slopes[at] = dot_nt(vals[:, wide], two_heads(go[:, wide]))
        for e, kr in enumerate((krlo, krhi)):
            key = jnp.concatenate([key_pair[:, lanes_of(e)], kr[...]], axis=1)
            query = jnp.concatenate([qn_pair[:, lanes_of(e)], qr_pair], axis=1)
            scores = dot_nt(key, query)
            top = None
            for i, block in enumerate(blocks):
                piece = scores[block]
                if i == STEPS:
                    piece = piece + bias[...]
                raw[at, block, lanes_of(e)] = piece
                high = fold(piece, jnp.max)
                if i < STEPS:
                    high = high + flags[i]
                top = high if top is None else jnp.maximum(top, high)
            tops[at, :, lanes_of(e)] = jnp.broadcast_to(jnp.max(top, axis=0, keepdims=True), (8, group))

    def softmax_pair(j, at):
        for e in range(2):
            lanes = lanes_of(e)
            mine = at_pair(2 * j + e, group)
            top = tops[at, 0:1, lanes] * rate
            shift = [top - flags[i] if i < STEPS else top for i in range(STEPS + 1)]
            total = None
            for i, block in enumerate(blocks):
                part = fold(jnp.exp2(raw[at, block, lanes] * rate - shift[i]), jnp.sum)
                total = part if total is None else total + part
            norm = jnp.log2(jnp.sum(total, axis=0, keepdims=True))
            delta = None
            for i, block in enumerate(blocks):
                probs = jnp.exp2(raw[at, block, lanes] * rate - (shift[i] + norm))
                weights[block, mine] = probs.astype(BF)
                part = fold(probs * slopes[at, block, lanes], jnp.sum)
                delta = part if delta is None else delta + part
            delta = jnp.sum(delta, axis=0, keepdims=True)
            for block in blocks:
                slope = ((slopes[at, block, lanes] - delta) * scale).astype(BF)
                slopes_grad[block, mine] = weights[block, mine] * slope

    score_pair(0, 0)
    score_pair(1, 1)
    softmax_pair(0, 0)

    def pair_step(j, carry):
        now = lax.rem(j, 2)
        score_pair(j + 1, 1 - now)
        softmax_pair(j, now)
        return carry

    lax.fori_loop(1, pairs - 1, pair_step, 0, unroll=min(6, pairs - 2))
    last = (pairs - 1) % 2
    softmax_pair(pairs - 1, last)

    def terms_of(k):
        at = pl.ds(pl.multiple_of((STEPS - k) * group, group), group)
        for j in range(pairs):
            mine = slice(j * 2 * group, (j + 1) * 2 * group)
            wide = slice(j * 2 * NOPE, (j + 1) * 2 * NOPE)
            dkeys[:, wide] = jnp.dot(
                slopes_grad[at, mine], two_heads(qn[:, wide]), preferred_element_type=F32
            ).astype(BF)
            dvals[:, wide] = jnp.dot(
                weights[at, mine], two_heads(go[:, wide]), preferred_element_type=F32
            ).astype(BF)
        content = jnp.dot(dkeys[...], kut[...], preferred_element_type=F32)
        content = content + jnp.dot(dvals[...], vut[...], preferred_element_type=F32)
        both = jnp.dot(slopes_grad[at, :], qrs[...], preferred_element_type=F32)
        rope = both[:, :ROPE] + both[:, ROPE:]
        return content.reshape(n_head, rows, RANK), rope.reshape(n_head, rows, ROPE)

    def put(ref, k):
        content, rope = terms_of(k)
        ref[:, :, :RANK] = content.astype(ref.dtype)
        ref[:, :, RANK:] = rope.astype(ref.dtype)

    order = [*range(n_head - 1, 0, -1), 0]
    chunk = near
    back_k, own_k = jnp.where(even, 1, 3), jnp.where(even, 3, 1)
    far_who = jnp.where(even, c - 3, c - 1)

    def send_part(i, slot, who, t):
        return pltpu.make_async_remote_copy(
            src_ref=parts.at[i, chunk(t)], dst_ref=got.at[slot, chunk(t)], send_sem=ps_sem.at[i],
            recv_sem=got_sem.at[slot, chunk(t)], device_id=(who, h), device_id_type=MESH,
        )

    def part_back(t):
        return send_part(0, FOR_BACK, partner, t)

    def part_next(t):
        return send_part(2, FROM_NEXT, c - 2, t)

    def part_own(t):
        return send_part(1, FOR_OWN, far_who, t)

    def wait_part(slot, t):
        send_part(0, slot, partner, t).wait_recv()

    def put_own_part():
        put(parts.at[1], own_k)

        @pl.when(c >= own_k)
        def _():
            for t in order:
                part_own(t).start()

    own_first = (lax.rem(c, 4) == 2) & (c >= own_k)
    put(parts.at[0], back_k)

    @pl.when(c >= back_k)
    def _():
        for t in order:
            part_back(t).start()

    pl.when(own_first)(put_own_part)

    put(back, 2)

    @pl.when(c >= 2)
    def _():
        for t in order:
            wait_part(FOR_BACK, t)
            parts[2, chunk(t)] = (back[chunk(t)] + got[FOR_BACK, chunk(t)].astype(F32)).astype(BF)
            part_next(t).start()

    pl.when(jnp.logical_not(own_first))(put_own_part)

    put(own, 0)

    def dq_step(j, carry):
        wide = at_pair(j, 2 * NOPE)
        key_pair = keys[:, wide]
        nope, rope = [], None
        for e, kr in enumerate((krlo, krhi)):
            key = jnp.concatenate([key_pair[:, e * NOPE : (e + 1) * NOPE], kr[...]], axis=1)
            both = dot_tn(slopes_grad[:, at_pair(2 * j + e, group)], key)
            nope.append(both[:, :NOPE])
            rope = both[:, NOPE:] if rope is None else rope + both[:, NOPE:]
        dqn[:, wide] = jnp.concatenate(nope, axis=1)
        dqr[:, at_pair(j, 2 * ROPE)] = rope
        return carry

    own_ok = even | (c + 3 < n_ctx)

    def scatter(t):
        return pltpu.make_async_remote_copy(
            src_ref=zparts.at[chunk(t)], dst_ref=zgot.at[h], send_sem=ws_sem,
            recv_sem=zgot_sem.at[h], device_id=(c, chunk(t)), device_id_type=MESH,
        )

    turns = len(order)
    for i, t in enumerate(order):
        first, last = ((pairs * (i + turns - 1)) // (2 * turns - 2) if i else 0), (pairs * (i + turns)) // (2 * turns - 2)
        lax.fori_loop(first, min(last, pairs), dq_step, 0, unroll=True)

        @pl.when(own_ok)
        def _():
            wait_part(FOR_OWN, t)
            own[chunk(t)] += got[FOR_OWN, chunk(t)].astype(F32)

        @pl.when(c + 2 < n_ctx)
        def _():
            wait_part(FROM_NEXT, t)
            own[chunk(t)] += got[FROM_NEXT, chunk(t)].astype(F32)

        if t > 0:
            zparts[chunk(t)] = own[chunk(t)].astype(BF)
            scatter(t).start()

    total = own[h]
    for t in range(1, n_head):
        pltpu.make_async_remote_copy(
            src_ref=zparts.at[h], dst_ref=zgot.at[near(t)], send_sem=ws_sem,
            recv_sem=zgot_sem.at[near(t)], device_id=(c, near(t)), device_id_type=MESH,
        ).wait_recv()
        total = total + zgot[near(t)].astype(F32)
    dlat_ref[...] = total

    def sent(sem, count):
        pltpu.make_async_remote_copy(
            src_ref=win.at[0, pl.ds(0, count)], dst_ref=win.at[0, pl.ds(0, count)], send_sem=sem,
            recv_sem=win_sem.at[0, 0], device_id=(partner, h), device_id_type=MESH,
        ).wait_send()

    sent(ws_sem, n_head - 1)
    sent(zs_sem, n_head - 1)
    for ok, sem, count in (
        (c + 2 < n_ctx, as_sem, n_head),
        (b_ok, bs_sem, n_head),
        ((c >= 2) & even, cs_sem, late),
        ((c >= 2) & jnp.logical_not(even), cs_sem, n_head),
        (direct_ok, ds_sem, n_head - late),
        (c >= 2, ps_sem.at[2], n_head),
        (c >= back_k, ps_sem.at[0], n_head),
        (c >= own_k, ps_sem.at[1], n_head),
    ):

        @pl.when(ok)
        def _():
            sent(sem, count)


def write_out(a, b, c, a_hbm, b_hbm, c_hbm, sem):
    copies = [
        pltpu.make_async_copy(src, dst, sem.at[i])
        for i, (src, dst) in enumerate([(a, a_hbm), (b, b_hbm), (c, c_hbm)])
    ]
    for copy in copies:
        copy.start()
    for copy in copies:
        copy.wait()


def on_device(n_ctx, n_head, query_nope, query_rope, grad_out, latent, key_up, value_up, block_keep):
    rows, width = latent.shape
    group = query_nope.shape[0]
    span = group * (STEPS + 1)
    wide = query_nope.shape[1]
    rope_wide = query_rope.shape[1]
    heads = wide // NOPE
    assert block_keep.shape[1] == STEPS and n_ctx % 2 == 0 and heads % 2 == 0 and heads >= 4
    vmem, hbm = pl.BlockSpec(memory_space=pltpu.VMEM), pl.BlockSpec(memory_space=pl.ANY)
    dma = pltpu.SemaphoreType.DMA
    block = (n_head, rows, width)
    results = pl.pallas_call(
        functools.partial(kernel, n_ctx, n_head),
        out_shape=(
            pltpu.VMEM((group, wide), F32),
            pltpu.VMEM((group, rope_wide), F32),
            pltpu.VMEM((rows, width), F32),
        ),
        in_specs=[hbm, hbm, hbm, hbm, hbm, hbm, hbm],
        out_specs=(vmem, vmem, vmem),
        scratch_shapes=[
            pltpu.SMEM(block_keep.shape, block_keep.dtype),
            pltpu.VMEM((STEPS + 1,) + block, BF),
            pltpu.VMEM((group, wide), BF),
            pltpu.VMEM((group, rope_wide), BF),
            pltpu.VMEM((group, wide), BF),
            pltpu.VMEM((RANK, wide), BF),
            pltpu.VMEM((RANK, wide), BF),
            pltpu.VMEM((wide, RANK), BF),
            pltpu.VMEM((wide, RANK), BF),
            pltpu.VMEM((heads * group, 2 * ROPE), BF),
            pltpu.VMEM((span, 2 * ROPE), BF),
            pltpu.VMEM((span, 2 * ROPE), BF),
            pltpu.VMEM((group, group), F32),
            pltpu.VMEM((span, wide), BF),
            pltpu.VMEM((span, wide), BF),
            pltpu.VMEM((group, wide), BF),
            pltpu.VMEM((group, wide), BF),
            pltpu.VMEM((span, heads * group), BF),
            pltpu.VMEM((2, span, 2 * group), F32),
            pltpu.VMEM((2, 8, 2 * group), F32),
            pltpu.VMEM((2, span, 2 * group), F32),
            pltpu.VMEM((span, heads * group), BF),
            pltpu.VMEM(block, F32),
            pltpu.VMEM(block, F32),
            pltpu.VMEM((3,) + block, BF),
            pltpu.VMEM((3,) + block, BF),
            pltpu.VMEM(block, BF),
            pltpu.VMEM(block, BF),
            dma((5,)),
            dma(()),
            dma(()),
            dma(()),
            dma(()),
            dma(()),
            dma(()),
            dma(()),
            dma((STEPS + 1, n_head)),
            dma((3,)),
            dma((3, n_head)),
            dma(()),
            dma((n_head,)),
        ],
        compiler_params=pltpu.CompilerParams(collective_id=0, has_side_effects=True),
        name="latent_attention_grads",
    )(block_keep, latent, query_nope, query_rope, grad_out, key_up, value_up)

    return pl.pallas_call(
        write_out,
        out_shape=tuple(jax.ShapeDtypeStruct(r.shape, r.dtype) for r in results),
        in_specs=[vmem] * 3,
        out_specs=[hbm] * 3,
        scratch_shapes=[dma((3,))],
        name="write_out",
    )(*(pltpu.with_memory_space_constraint(r, pltpu.VMEM) for r in results))


def solution(mesh):
    placed = (
        P("ctx", "head"),
        P("ctx", "head"),
        P("ctx", "head"),
        P(("ctx", "head"), None),
        P(None, "head"),
        P(None, "head"),
        P("ctx", None),
    )
    return jax.shard_map(
        functools.partial(on_device, mesh.shape["ctx"], mesh.shape["head"]),
        mesh=mesh,
        in_specs=placed,
        out_specs=(P("ctx", "head"), P("ctx", "head"), P(("ctx", "head"), None)),
        check_vma=False,
    )
```
